32 devices in a mesh: row: 8 (over y, x, core), col: 4 (over z).
Axes of the slice: x: 2, y: 2, z: 4, core: 2. Of those that a mesh axis runs over, the one named last changes fastest.
Arguments:
- inputs: int32 [8, 128, 128], replicated, may hold values 0 or 1
- targets: int32 [8, 128, 128], replicated, may hold values 0 or 1
- initial_spikes: int32 [128, 128, 128], P(None, 'row'), may hold values 0 or 1
- w_in: bfloat16 [128, 128, 128], P(None, 'row'), may hold values from -0.5 to 0.5
- w_rec: bfloat16 [128, 128, 128, 128], P(None, 'col', 'row'), may hold values from -0.046875 to 0.046875
- w_out: bfloat16 [128, 128, 128], P('row'), may hold values from -0.046875 to 0.046875
- feedback: bfloat16 [128, 128, 128], P(None, 'row')
- adapt_gain: float32 [128, 128], P('row'), may hold values from 0.1 to 2
- adapt_decay: float32 [128, 128], P('row'), may hold values from 0.8 to 0.99
Outputs:
- readout: float32 [8, 128, 128], replicated
- grad_clipped: float32 [128, 128, 128, 128], P(None, 'col', 'row')
The draws below stay inside these ranges and needn't reach their ends.
All inputs are finite; a program needn't handle non-finite values. No bound on the sum of `initial_spikes` on one device may be relied on, other than what follows from the above.
Results may differ from the reference program's by a relative error of at most 0.0015.
Values may be sent and summed in bfloat16 or wider, within the bound.
No kernel may reach another device: no remote copies, remote signals or barrier semaphores. Data moves between devices by JAX's collectives and lax.ppermute only.
A program may use at most 128 MiB of HBM per device.

```python
import math
import jax
import jax.numpy as jnp
from jax import lax

NA = 128
NB = 128
NIN = 128
K = 128
T_SIZE = 8
B = 128


def draw_feedback(key, part):
    position = jnp.arange(NA, dtype=jnp.float32) / max(NA - 1, 1)
    ramp = 1.0 + 2.0 * position
    base = jax.random.normal(key, (K, NA, NB), jnp.float32)
    ramp = ramp / jnp.sqrt(jnp.mean(ramp * ramp))
    values = base * ramp[None, :, None] * K ** (-0.5)
    return values.astype(jnp.bfloat16)


def plant(drawn, own_key, low, top_value):
    place = [jax.random.randint(jax.random.fold_in(own_key, axis), (), 0, length) for axis, length in enumerate(drawn.shape)]
    widest = drawn.shape.index(max(drawn.shape))
    next_to = place[:widest] + [(place[widest] + 1) % drawn.shape[widest]] + place[widest + 1:]
    return drawn.at[tuple(place)].set(low).at[tuple(next_to)].set(top_value)


def steps_of(key, extent, split, least, largest):
    level, own = 1.0, jax.random.fold_in(key, 6)
    for dim, shards_of in split:
        steps = jnp.exp(jax.random.uniform(jax.random.fold_in(own, dim), (shards_of,), jnp.float32, least / len(split), largest / len(split)))
        level = level * jnp.repeat(steps, extent[dim] // shards_of).reshape([-1 if axis == dim else 1 for axis in range(len(extent))])
    return level


def centred(key, shape, deviation, limit, shards=(), kind=jnp.bfloat16):
    gain = steps_of(key, shape, shards, -0.22, 0.18) if shards else 1.0
    values = jax.random.normal(key, shape, jnp.float32) * deviation * gain
    return jnp.minimum(jnp.maximum(values, -limit), limit).astype(kind)


def setup_inputs(seed: int = 0) -> dict:
    arg_keys = jax.random.split(jax.random.key(seed), 10)
    inputs = plant((jax.random.randint(arg_keys[0], (T_SIZE, B, NIN), 0, 5) < 1).astype(jnp.int32), jax.random.fold_in(arg_keys[0], 1), 0, 1)
    targets = plant((jax.random.randint(arg_keys[1], (T_SIZE, B, K), 0, 4) < 1).astype(jnp.int32), jax.random.fold_in(arg_keys[1], 1), 0, 1)
    initial_spikes = plant((jax.random.randint(arg_keys[2], (B, NA, NB), 0, 2) < 1).astype(jnp.int32), jax.random.fold_in(arg_keys[2], 1), 0, 1)
    w_in = centred(arg_keys[3], (NIN, NA, NB), NIN ** -0.5, 0.5, ((1, 8),))
    w_rec = centred(arg_keys[4], (NA, NB, NA, NB), (NA * NB) ** -0.5, 0.046875, ((1, 4), (2, 8)))
    w_out = centred(arg_keys[5], (NA, NB, K), (NA * NB) ** -0.5, 0.046875, ((0, 8),))
    feedback = draw_feedback(jax.random.fold_in(arg_keys[9], 71), 0)
    adapt_gain = jnp.clip(jnp.exp(math.log(2.0) - 2.9957323 * jax.random.uniform(arg_keys[7], (NA, NB), jnp.float32) ** steps_of(arg_keys[7], (NA, NB), ((0, 8),), -0.2, 0.2)), 0.1, 2.0)
    adapt_decay = jnp.clip(0.8 + 0.19 * jax.random.uniform(arg_keys[8], (NA, NB), jnp.float32) ** steps_of(arg_keys[8], (NA, NB), ((0, 8),), -0.2, 0.2), 0.8, 0.99)
    return {"inputs": inputs, "targets": targets, "initial_spikes": initial_spikes, "w_in": w_in, "w_rec": w_rec, "w_out": w_out, "feedback": feedback, "adapt_gain": adapt_gain, "adapt_decay": adapt_decay}


cellular_leak_multiplier = 0.8
readout_decay = 0.8

def reference(inputs, targets, initial_spikes, w_in, w_rec, w_out, feedback, adapt_gain, adapt_decay):
    neurons = NA * NB
    rows_all = T_SIZE * B
    external = jnp.dot(inputs.reshape(rows_all, NIN).astype(jnp.bfloat16), w_in.reshape(NIN, neurons), preferred_element_type=jnp.float32).reshape(T_SIZE, B, neurons)
    weights = w_rec.reshape(neurons, neurons)
    coupling_magnitude = adapt_gain.reshape(neurons)
    retention = adapt_decay.reshape(neurons)

    def advance(state, drive_now):
        pulse_output, cellular_charge, barrier_shift_amount, sender_trace = state
        spike_float = pulse_output.astype(jnp.float32)
        sender_trace = cellular_leak_multiplier * sender_trace + spike_float
        current = drive_now + jnp.dot(pulse_output, weights, preferred_element_type=jnp.float32)
        cellular_charge = cellular_leak_multiplier * cellular_charge + current - spike_float
        barrier_shift_amount = retention * barrier_shift_amount + spike_float
        present_emission_frequency = jax.nn.sigmoid(cellular_charge - 1.0 - coupling_magnitude * barrier_shift_amount)
        surrogate_slope = present_emission_frequency * (1.0 - present_emission_frequency)
        pulse_output = present_emission_frequency.astype(jnp.bfloat16)
        return ((pulse_output, cellular_charge, barrier_shift_amount, sender_trace), (sender_trace.astype(jnp.bfloat16), surrogate_slope, pulse_output))
    zeros = jnp.zeros((B, neurons), jnp.float32)
    start_state = (initial_spikes.reshape(B, neurons).astype(jnp.bfloat16), zeros, zeros, zeros)
    _, (traces, slopes, spikes) = lax.scan(advance, start_state, external)
    projected = jnp.dot(spikes.reshape(rows_all, neurons), w_out.reshape(neurons, K), preferred_element_type=jnp.float32).reshape(T_SIZE, B, K)

    def smooth(level, incoming):
        level = readout_decay * level + incoming
        return (level, level)
    _, readout = lax.scan(smooth, jnp.zeros((B, K), jnp.float32), projected)
    errors = (jax.nn.sigmoid(readout) - targets.astype(jnp.float32)).reshape(rows_all, K)
    err_high = errors.astype(jnp.bfloat16)
    err_low = (errors - err_high.astype(jnp.float32)).astype(jnp.bfloat16)
    fb_flat = feedback.reshape(K, neurons)
    signal = jnp.dot(err_high, fb_flat, preferred_element_type=jnp.float32) + jnp.dot(err_low, fb_flat, preferred_element_type=jnp.float32)
    signal = signal.reshape(T_SIZE, B, neurons)
    weighted = signal * slopes
    decays = retention - slopes * coupling_magnitude

    def backward(carried, inputs_now):
        weighted_now, decay_now = inputs_now
        return (weighted_now + decay_now * carried, carried)
    _, future = lax.scan(backward, zeros, (weighted, decays), reverse=True)
    factors = (weighted - coupling_magnitude * slopes * future).astype(jnp.bfloat16)
    grad = lax.dot_general(traces.reshape(rows_all, neurons), factors.reshape(rows_all, neurons), (((0,), (0,)), ((), ())), preferred_element_type=jnp.float32)
    squares = jnp.sum(grad * grad)
    clip_factor = jnp.minimum(1.0, NA * NB / 16.0 / jnp.sqrt(squares + 1e-06))
    return (readout, (grad * clip_factor).reshape(NA, NB, NA, NB))
```

```python
import functools
import jax
import jax.numpy as jnp
from jax import lax
from jax.experimental import pallas as pl
from jax.experimental.pallas import tpu as pltpu
from jax.sharding import PartitionSpec as P

NA = 128
NB = 128


cellular_leak_multiplier = 0.8
readout_decay = 0.8
f32 = jnp.float32
bf16 = jnp.bfloat16
LANES = 128


def params(mib):
    return pltpu.CompilerParams(vmem_limit_bytes=mib << 20)


def cost(flops, moved=0):
    return pl.CostEstimate(flops=int(flops), transcendentals=0, bytes_accessed=int(moved))


def whole_spec(shape):
    return pl.BlockSpec(shape, lambda *_: (0,) * len(shape))


SCALARS = pl.BlockSpec(memory_space=pltpu.SMEM)


def flatten_weights(w):
    senders, rows, width = w.shape
    block = min(256, senders)

    def kernel(w_ref, o_ref):
        o_ref[...] = w_ref[...].reshape(block, rows * width)

    return pl.pallas_call(
        kernel,
        grid=(senders // block,),
        in_specs=[pl.BlockSpec((block, rows, width), lambda i: (i, 0, 0))],
        out_specs=pl.BlockSpec((block, rows * width), lambda i: (i, 0)),
        out_shape=jax.ShapeDtypeStruct((senders, rows * width), bf16),
        compiler_params=params(40),
        cost_estimate=cost(w.size * 500, w.size * 4),
        name="flatten_weights",
    )(w)


def step_matmul(where, pieces, weights, groups, own):
    batch, part = pieces[0].shape
    senders, receivers = weights.shape
    tile = LANES // own
    width = receivers // (part // own)
    lanes = tile * width
    count = len(pieces)

    def kernel(where_ref, *refs):
        piece_refs, w_ref = refs[:count], refs[count]
        spikes_ref, outs, pool = refs[count + 1], refs[count + 2 : count + 2 + groups], refs[-1]
        row, col = where_ref[0], where_ref[1]

        @pl.when(pl.program_id(0) == 0)
        def _():
            for k in range(count):
                start = pl.multiple_of((row ^ k) * part, part)
                spikes_ref[:, pl.ds(start, part)] = piece_refs[k][...]

        sums = jnp.dot(spikes_ref[...], w_ref[...], preferred_element_type=f32)
        for c in range(groups):
            pool[c] = jnp.concatenate(
                [sums[:, i * width + c * own : i * width + (c + 1) * own] for i in range(tile)], axis=1
            )
        for k in range(groups):
            outs[k][...] = pool[col ^ k].astype(outs[k].dtype)

    return pl.pallas_call(
        kernel,
        grid=(receivers // lanes,),
        in_specs=[SCALARS]
        + [whole_spec((batch, part))] * count
        + [pl.BlockSpec((senders, lanes), lambda g: (0, g))],
        out_specs=[whole_spec((batch, senders))] + [pl.BlockSpec((batch, LANES), lambda g: (0, g))] * groups,
        out_shape=[jax.ShapeDtypeStruct((batch, senders), bf16)]
        + [jax.ShapeDtypeStruct((batch, part), f32 if k == 0 else bf16) for k in range(groups)],
        scratch_shapes=[pltpu.VMEM((groups, batch, LANES), f32)],
        compiler_params=params(40),
        cost_estimate=cost(2 * batch * weights.size, 2 * weights.size),
        name="step_matmul",
    )(where, *pieces, weights)


def step_state(t, partials, external, spikes, voltage, fatigue, gain, decay):
    batch, part = spikes.shape
    count = len(partials)
    first = voltage is None
    states = [] if first else [voltage, fatigue]

    def kernel(*refs):
        part_refs, drive_ref, s_ref = refs[:count], refs[count], refs[count + 1]
        gain_ref, decay_ref = refs[count + 2], refs[count + 3]
        s_out, v_out, u_out = refs[-3:]
        current = drive_ref[0]
        for ref in part_refs:
            current = current + ref[...].astype(f32)
        s = s_ref[...].astype(f32)
        v, u = current - s, s
        if not first:
            v = cellular_leak_multiplier * refs[count + 4][...] + v
            u = decay_ref[...] * refs[count + 5][...] + u
        f = jax.nn.sigmoid(v - 1.0 - gain_ref[...] * u)
        s_out[...] = f.astype(bf16)
        v_out[...] = v
        u_out[...] = u

    full = whole_spec((batch, part))
    line = whole_spec((1, part))
    return pl.pallas_call(
        kernel,
        grid=(1,),
        in_specs=[full] * count
        + [pl.BlockSpec((1, batch, part), lambda g: (t, 0, 0)), full, line, line]
        + [full] * len(states),
        out_specs=[full] * 3,
        out_shape=[jax.ShapeDtypeStruct((batch, part), d) for d in (bf16, f32, f32)],
        compiler_params=params(24),
        cost_estimate=cost(2000 * spikes.size),
        name="step_state",
    )(*partials, external, spikes, gain, decay, *states)


def make_traces(gathered):
    steps = len(gathered)
    batch, senders = gathered[0].shape
    rows_all = steps * batch
    block = min(512, senders)

    def kernel(*refs):
        traces_ref, gram_ref, held = refs[steps], refs[steps + 1], refs[steps + 2]
        trace = jnp.zeros((batch, block), f32)
        for t in range(steps):
            trace = cellular_leak_multiplier * trace + refs[t][...].astype(f32)
            held[t * batch : (t + 1) * batch, :] = trace.astype(bf16)
        x = held[...]
        traces_ref[...] = x.T
        gram = lax.dot_general(x, x, (((1,), (1,)), ((), ())), preferred_element_type=f32)

        @pl.when(pl.program_id(0) == 0)
        def _():
            gram_ref[...] = gram

        @pl.when(pl.program_id(0) > 0)
        def _():
            gram_ref[...] += gram

    return pl.pallas_call(
        kernel,
        grid=(senders // block,),
        in_specs=[pl.BlockSpec((batch, block), lambda j: (0, j))] * steps,
        out_specs=[pl.BlockSpec((block, rows_all), lambda j: (j, 0)), whole_spec((rows_all, rows_all))],
        out_shape=[
            jax.ShapeDtypeStruct((senders, rows_all), bf16),
            jax.ShapeDtypeStruct((rows_all, rows_all), f32),
        ],
        scratch_shapes=[pltpu.VMEM((rows_all, block), bf16)],
        compiler_params=params(48),
        cost_estimate=cost(2 * rows_all * rows_all * senders, 4 * rows_all * senders),
        name="make_traces",
    )(*gathered)


def make_factors(where, projected, targets, feedback, fired, gain, decay, gram, groups, own):
    steps, batch, channels = targets.shape
    rows_all = steps * batch
    receivers = feedback.shape[1]
    width = groups * own
    tile = LANES // own
    lanes = tile * width
    share = projected[0].shape[0]
    count, held = len(projected), len(fired)
    per = fired[0].shape[1] // batch

    def kernel(where_ref, *refs):
        proj_refs, refs = refs[:count], refs[count:]
        targets_ref, feedback_ref, refs = refs[0], refs[1], refs[2:]
        fired_refs, refs = refs[:held], refs[held:]
        gain_ref, decay_ref, gram_ref, readout_ref, factors_ref, squares_ref, pool, pair, own_gram = refs
        g = pl.program_id(0)

        @pl.when(g == 0)
        def _():
            row = where_ref[0]
            for k in range(count):
                pool[row ^ k] = proj_refs[k][...]
            level = jnp.zeros((batch, channels), f32)
            for t in range(steps):
                level = readout_decay * level + pool[t // share, t % share]
                readout_ref[t] = level
                error = jax.nn.sigmoid(level) - targets_ref[t].astype(f32)
                high = error.astype(bf16)
                low = (error - high.astype(f32)).astype(bf16)
                pair[t * batch : (t + 1) * batch, :channels] = high
                pair[t * batch : (t + 1) * batch, channels:] = low

        twice = jnp.concatenate([feedback_ref[...], feedback_ref[...]], axis=0)
        future = jnp.zeros((batch, lanes), f32)
        for t in reversed(range(steps)):
            signal = jnp.dot(pair[t * batch : (t + 1) * batch, :], twice, preferred_element_type=f32)
            ref, at = fired_refs[t // per], (t % per) * batch
            f = jnp.concatenate(
                [
                    ref[c, at : at + batch, i * own : (i + 1) * own]
                    for i in range(tile)
                    for c in range(groups)
                ],
                axis=1,
            ).astype(f32)
            slope = f * (1.0 - f)
            weighted = signal * slope
            strength = gain_ref[...] * slope
            factors_ref[t * batch : (t + 1) * batch, :] = (weighted - strength * future).astype(bf16)
            future = weighted + (decay_ref[...] - strength) * future
        x = factors_ref[...]
        part = lax.dot_general(x, x, (((1,), (1,)), ((), ())), preferred_element_type=f32)

        @pl.when(g == 0)
        def _():
            own_gram[...] = part

        @pl.when(g > 0)
        def _():
            own_gram[...] += part

        @pl.when(g == pl.num_programs(0) - 1)
        def _():
            squares_ref[...] = jnp.full(squares_ref.shape, jnp.sum(own_gram[...] * gram_ref[...]), f32)

    return pl.pallas_call(
        kernel,
        grid=(receivers // lanes,),
        in_specs=[SCALARS]
        + [whole_spec(projected[0].shape)] * count
        + [whole_spec(targets.shape), pl.BlockSpec((channels, lanes), lambda g: (0, g))]
        + [pl.BlockSpec((groups, per * batch, LANES), lambda g: (0, 0, g))] * held
        + [pl.BlockSpec((1, lanes), lambda g: (0, g))] * 2
        + [whole_spec(gram.shape)],
        out_specs=[
            whole_spec(targets.shape),
            pl.BlockSpec((rows_all, lanes), lambda g: (0, g)),
            whole_spec((8, LANES)),
        ],
        out_shape=[
            jax.ShapeDtypeStruct(targets.shape, f32),
            jax.ShapeDtypeStruct((rows_all, receivers), bf16),
            jax.ShapeDtypeStruct((8, LANES), f32),
        ],
        scratch_shapes=[
            pltpu.VMEM((count,) + projected[0].shape, f32),
            pltpu.VMEM((rows_all, 2 * channels), bf16),
            pltpu.VMEM((rows_all, rows_all), f32),
        ],
        compiler_params=params(56),
        cost_estimate=cost(4 * rows_all * rows_all * receivers),
        name="make_factors",
    )(where, *projected, targets, feedback, *fired, gain, decay, gram)


def make_gradient(squares, limit, traces, factors, rows):
    senders, rows_all = traces.shape
    receivers = factors.shape[1]
    width = receivers // rows
    block = min(256, senders)

    def kernel(squares_ref, traces_ref, factors_ref, o_ref):
        total = squares_ref[0:1, 0:1]
        clip = jnp.minimum(1.0, limit / jnp.sqrt(total + 1e-06))
        product = jnp.dot(traces_ref[...], factors_ref[...], preferred_element_type=f32) * clip
        out = o_ref.reshape(block * rows, width)
        for i in range(rows):
            out[pl.ds(i, block, stride=rows), :] = product[:, i * width : (i + 1) * width]

    return pl.pallas_call(
        kernel,
        grid=(senders // block,),
        in_specs=[
            whole_spec(squares.shape),
            pl.BlockSpec((block, rows_all), lambda i: (i, 0)),
            whole_spec(factors.shape),
        ],
        out_specs=pl.BlockSpec((block, rows, width), lambda i: (i, 0, 0)),
        out_shape=jax.ShapeDtypeStruct((senders, rows, width), f32),
        compiler_params=params(48),
        cost_estimate=cost(2 * senders * rows_all * receivers, 4 * senders * receivers),
        name="make_gradient",
    )(squares, traces, factors)


def body(row_count, col_count, inputs, targets, initial_spikes, w_in, w_rec, w_out, feedback, adapt_gain, adapt_decay):
    steps, batch, channels = inputs.shape
    own = w_rec.shape[1]
    rows = w_rec.shape[2]
    width = w_rec.shape[3]
    part = rows * own
    row, col = lax.axis_index("row"), lax.axis_index("col")
    where = jnp.stack([row, col]).astype(jnp.int32)

    def swap(x, axis, k):
        size = row_count if axis == "row" else col_count
        return lax.ppermute(x, axis, [(d, d ^ k) for d in range(size)])

    def gather_row(x):
        even = {0: x}
        for k in range(2, row_count, 2):
            even[k] = swap(x, "row", k)
        pieces = []
        for k in range(0, row_count, 2):
            pieces += [even[k], swap(even[k], "row", 1)]
        return pieces

    def mine(array, axis):
        return lax.dynamic_slice_in_dim(array, col * own, own, axis)

    weights = flatten_weights(w_rec.reshape(-1, rows, width))
    external = jnp.dot(
        inputs.reshape(steps * batch, channels).astype(bf16),
        mine(w_in, 2).reshape(channels, part),
        preferred_element_type=f32,
    ).reshape(steps, batch, part)
    gain = mine(adapt_gain, 1).reshape(1, part)
    decay = mine(adapt_decay, 1).reshape(1, part)
    readout_own = mine(w_out, 1).reshape(part, -1)
    spikes = mine(initial_spikes, 2).astype(bf16).reshape(batch, part)

    voltage = fatigue = None
    gathered, fired, projected, pending = [], [], [], []
    for t in range(steps):
        spikes_all, kept, *leaving = step_matmul(where, gather_row(spikes), weights, col_count, own)
        gathered.append(spikes_all)
        arrived = [swap(x, "col", k + 1) for k, x in enumerate(leaving)]
        spikes, voltage, fatigue = step_state(
            t, [kept] + arrived, external, spikes, voltage, fatigue, gain, decay
        )
        projected.append(jnp.dot(spikes, readout_own, preferred_element_type=f32))
        pending.append(spikes)
        if len(pending) == 2 or t == steps - 1:
            fired.append(lax.all_gather(jnp.concatenate(pending), "col", axis=0))
            pending = []
    traces, gram = make_traces(gathered)

    outputs_n = readout_own.shape[1]
    shares = jnp.stack(projected).reshape(row_count, steps // row_count, batch, outputs_n)
    total = lax.dynamic_index_in_dim(shares, row, 0, keepdims=False)
    for k in range(1, row_count):
        total = total + swap(lax.dynamic_index_in_dim(shares, row ^ k, 0, keepdims=False), "row", k)
    over_cols = total
    for k in range(1, col_count):
        over_cols = over_cols + swap(total, "col", k)
    readout, factors, squares = make_factors(
        where,
        gather_row(over_cols),
        targets,
        feedback.reshape(outputs_n, -1),
        fired,
        adapt_gain.reshape(1, -1),
        adapt_decay.reshape(1, -1),
        gram,
        col_count,
        own,
    )
    total = squares
    for k in range(1, row_count):
        total = total + swap(squares, "row", k)
    norm = total
    for k in range(1, col_count):
        norm = norm + swap(total, "col", k)
    limit = w_rec.shape[0] * width / 16.0
    return (readout, make_gradient(norm, limit, traces, factors, rows).reshape(w_rec.shape))


def plain(inputs, targets, initial_spikes, w_in, w_rec, w_out, feedback, adapt_gain, adapt_decay):
    steps_count, batch, channels = inputs.shape
    own_cols = w_rec.shape[1]
    rows_loc = w_rec.shape[2]
    entire_column_set = w_rec.shape[3]
    col_start = lax.axis_index("col") * own_cols
    rows_all = steps_count * batch

    def own_part(array, axis_dim):
        return lax.dynamic_slice_in_dim(array, col_start, own_cols, axis_dim)

    def select_cols(array, axis_dim):
        return own_part(array, axis_dim)

    def combine_currents(partial_value):
        return lax.psum_scatter(partial_value, "col", scatter_dimension=2, tiled=True)

    weights = w_rec.reshape(w_rec.shape[0] * own_cols, rows_loc * entire_column_set)
    w_in_loc = select_cols(w_in, 2)
    state_cols = w_in_loc.shape[2]
    external = jnp.dot(
        inputs.reshape(rows_all, channels).astype(jnp.bfloat16),
        w_in_loc.reshape(channels, -1),
        preferred_element_type=jnp.float32,
    ).reshape(steps_count, batch, rows_loc, state_cols)
    coupling_magnitude = select_cols(adapt_gain, 1)
    retention = select_cols(adapt_decay, 1)
    start_spikes = select_cols(initial_spikes, 2).astype(jnp.bfloat16)

    def advance(state, drive_now):
        pulse_output, cellular_charge, barrier_shift_amount, sender_trace = state
        arrivals = lax.all_gather(pulse_output, "row", axis=1, tiled=True).reshape(batch, -1)
        sender_trace = cellular_leak_multiplier * sender_trace + arrivals.astype(jnp.float32)
        partial_value = jnp.dot(arrivals, weights, preferred_element_type=jnp.float32).reshape(
            batch, rows_loc, entire_column_set
        )
        current = drive_now + combine_currents(partial_value)
        spike_float = pulse_output.astype(jnp.float32)
        cellular_charge = cellular_leak_multiplier * cellular_charge + current - spike_float
        barrier_shift_amount = retention * barrier_shift_amount + spike_float
        present_emission_frequency = jax.nn.sigmoid(
            cellular_charge - 1.0 - coupling_magnitude * barrier_shift_amount
        )
        surrogate_slope = present_emission_frequency * (1.0 - present_emission_frequency)
        pulse_output = present_emission_frequency.astype(jnp.bfloat16)
        return (
            (pulse_output, cellular_charge, barrier_shift_amount, sender_trace),
            (sender_trace.astype(jnp.bfloat16), surrogate_slope, pulse_output),
        )

    zeros = jnp.zeros((batch, rows_loc, state_cols), jnp.float32)
    trace_zero = jnp.zeros((batch, weights.shape[0]), jnp.float32)
    _, (traces, slopes, spikes) = lax.scan(
        advance, (start_spikes, zeros, zeros, trace_zero), external
    )
    readout_loc = own_part(w_out, 1).reshape(rows_loc * own_cols, -1)
    projected = lax.psum(
        jnp.dot(spikes.reshape(rows_all, -1), readout_loc, preferred_element_type=jnp.float32),
        ("row", "col"),
    )
    outputs_n = readout_loc.shape[1]
    projected = projected.reshape(steps_count, batch, outputs_n)

    def smooth(level, incoming):
        level = readout_decay * level + incoming
        return (level, level)

    _, readout = lax.scan(smooth, jnp.zeros((batch, outputs_n), jnp.float32), projected)
    errors = (jax.nn.sigmoid(readout) - targets.astype(jnp.float32)).reshape(rows_all, outputs_n)
    err_high = errors.astype(jnp.bfloat16)
    err_low = (errors - err_high.astype(jnp.float32)).astype(jnp.bfloat16)
    feedback_loc = select_cols(feedback, 2).reshape(outputs_n, -1)
    signal = jnp.dot(err_high, feedback_loc, preferred_element_type=jnp.float32) + jnp.dot(
        err_low, feedback_loc, preferred_element_type=jnp.float32
    )
    signal = signal.reshape(steps_count, batch, rows_loc, state_cols)
    weighted = signal * slopes
    decays = retention - slopes * coupling_magnitude

    def backward(carried, inputs_now):
        weighted_now, decay_now = inputs_now
        return (weighted_now + decay_now * carried, carried)

    _, future = lax.scan(backward, zeros, (weighted, decays), reverse=True)
    factors = (weighted - coupling_magnitude * slopes * future).astype(jnp.bfloat16)
    traces_flat = traces.reshape(rows_all, -1)
    pieces = lax.all_gather(
        factors.reshape(rows_all, rows_loc, state_cols), "col", axis=2, tiled=True
    )
    product = lax.dot_general(
        traces_flat,
        pieces.reshape(rows_all, -1),
        (((0,), (0,)), ((), ())),
        preferred_element_type=jnp.float32,
    )
    grad = product.reshape(-1, rows_loc, pieces.shape[2])
    squares = lax.psum(jnp.sum(grad * grad), ("row", "col"))
    clip_factor = jnp.minimum(1.0, NA * NB / 16.0 / jnp.sqrt(squares + 1e-06))
    return (readout, (grad * clip_factor).reshape(w_rec.shape))


def power_of_two(n):
    return n > 1 and n & (n - 1) == 0


def solution(mesh):
    row_count, col_count = mesh.shape["row"], mesh.shape["col"]

    def choose(inputs, targets, initial_spikes, w_in, w_rec, *rest):
        steps, batch, channels = inputs.shape
        own, rows, width = w_rec.shape[1:]
        fits = (
            power_of_two(row_count)
            and power_of_two(col_count)
            and LANES % own == 0
            and (rows * own) % LANES == 0
            and rows % 8 == 0
            and width % LANES == 0
            and batch % 16 == 0
            and channels % LANES == 0
            and steps % row_count == 0
            and steps % 2 == 0
        )
        run = functools.partial(body, row_count, col_count) if fits else plain
        return run(inputs, targets, initial_spikes, w_in, w_rec, *rest)

    return jax.shard_map(
        choose,
        mesh=mesh,
        in_specs=(
            P(),
            P(),
            P(None, "row", None),
            P(None, "row", None),
            P(None, "col", "row", None),
            P("row", None, None),
            P(None, "row", None),
            P("row", None),
            P("row", None),
        ),
        out_specs=(P(), P(None, "col", "row", None)),
        check_vma=False,
    )
```

```python
import functools
import jax
import jax.numpy as jnp
from jax import lax
from jax.experimental import pallas as pl
from jax.experimental.pallas import tpu as pltpu
from jax.sharding import PartitionSpec as P

NA = 128
NB = 128


cellular_leak_multiplier = 0.8
readout_decay = 0.8
f32 = jnp.float32
bf16 = jnp.bfloat16
LANES = 128


def params(mib):
    return pltpu.CompilerParams(vmem_limit_bytes=mib << 20)


def cost(flops, moved=0):
    return pl.CostEstimate(flops=int(flops), transcendentals=0, bytes_accessed=int(moved))


def whole_spec(shape):
    return pl.BlockSpec(shape, lambda *_: (0,) * len(shape))


SCALARS = pl.BlockSpec(memory_space=pltpu.SMEM)


RESIDENT = pl.BlockSpec(memory_space=pltpu.VMEM)
UNREAD = pl.BlockSpec(memory_space=pl.ANY)


def flatten_weights(w, feedback, before):
    senders, rows, width = w.shape
    block = min(512, senders)

    def kernel(w_ref, feedback_ref, *refs):
        o_ref, flat_ref = refs[-2:]
        start = pl.multiple_of(pl.program_id(0) * block, block)
        o_ref[pl.ds(start, block), :] = w_ref[...].reshape(block, rows * width)

        @pl.when(pl.program_id(0) == 0)
        def _():
            flat_ref[...] = feedback_ref[...].reshape(flat_ref.shape)

    return pl.pallas_call(
        kernel,
        grid=(senders // block,),
        in_specs=[pl.BlockSpec((block, rows, width), lambda i: (i, 0, 0)), whole_spec(feedback.shape)]
        + [UNREAD] * len(before),
        out_specs=[RESIDENT, whole_spec((feedback.shape[0], rows * width))],
        out_shape=[
            pltpu.VMEM((senders, rows * width), bf16),
            jax.ShapeDtypeStruct((feedback.shape[0], rows * width), bf16),
        ],
        compiler_params=params(24),
        cost_estimate=cost(w.size * 500, w.size * 4),
        name="flatten_weights",
    )(w, feedback, *before)


def step_matmul(where, pieces, weights, groups, own):
    batch, part = pieces[0].shape
    senders, receivers = weights.shape
    tile = LANES // own
    width = receivers // (part // own)
    lanes = tile * width
    count = len(pieces)

    def kernel(where_ref, *refs):
        piece_refs, w_ref = refs[:count], refs[count]
        spikes_ref, outs, pool = refs[count + 1], refs[count + 2 : count + 2 + groups], refs[-1]
        row, col = where_ref[0], where_ref[1]
        for k in range(count):
            start = pl.multiple_of((row ^ k) * part, part)
            spikes_ref[:, pl.ds(start, part)] = piece_refs[k][...]

        def block(g, _):
            at = pl.ds(pl.multiple_of(g * lanes, lanes), lanes)
            sums = jnp.dot(spikes_ref[...], w_ref[:, at], preferred_element_type=f32)
            for c in range(groups):
                pool[c] = jnp.concatenate(
                    [sums[:, i * width + c * own : i * width + (c + 1) * own] for i in range(tile)], axis=1
                )
            to = pl.ds(pl.multiple_of(g * LANES, LANES), LANES)
            for k in range(groups):
                outs[k][:, to] = pool[col ^ k].astype(outs[k].dtype)
            return 0

        lax.fori_loop(0, receivers // lanes, block, 0)

    return pl.pallas_call(
        kernel,
        in_specs=[SCALARS] + [RESIDENT] * (count + 1),
        out_specs=[RESIDENT] * (groups + 1),
        out_shape=[pltpu.VMEM((batch, senders), bf16)]
        + [pltpu.VMEM((batch, part), f32 if k == 0 else bf16) for k in range(groups)],
        scratch_shapes=[pltpu.VMEM((groups, batch, LANES), f32)],
        compiler_params=params(8),
        cost_estimate=cost(2 * batch * weights.size),
        name="step_matmul",
    )(where, *pieces, weights)


def step_state(partials, spikes, voltage, fatigue, gain, decay):
    batch, part = spikes.shape
    count = len(partials)
    first = voltage is None
    states = [] if first else [voltage, fatigue]

    def kernel(*refs):
        s_ref, gain_ref, decay_ref = refs[count : count + 3]
        s_out, v_out, u_out = refs[-3:]
        current = refs[0][...]
        for ref in refs[1:count]:
            current = current + ref[...].astype(f32)
        s = s_ref[...].astype(f32)
        v, u = current - s, s
        if not first:
            v = cellular_leak_multiplier * refs[count + 3][...] + v
            u = decay_ref[...] * refs[count + 4][...] + u
        s_out[...] = jax.nn.sigmoid(v - 1.0 - gain_ref[...] * u).astype(bf16)
        v_out[...] = v
        u_out[...] = u

    return pl.pallas_call(
        kernel,
        in_specs=[RESIDENT] * (count + 3 + len(states)),
        out_specs=[RESIDENT] * 3,
        out_shape=[pltpu.VMEM((batch, part), d) for d in (bf16, f32, f32)],
        compiler_params=params(6),
        cost_estimate=cost(2000 * spikes.size),
        name="step_state",
    )(*partials, spikes, gain, decay, *states)


def step_trace(t, spikes_all, trace, before, spikes, readout_own, inputs, w_in_own, after):
    batch, senders = spikes_all.shape
    steps = len(before) + 1
    outputs_n = readout_own.shape[1]
    first = trace is None
    operands = [spikes_all, spikes, readout_own, inputs, w_in_own] + ([] if first else [trace]) + before
    chunk = min(512, senders)

    def kernel(*refs):
        s_ref, own_ref, readout_ref, inputs_ref, w_in_ref = refs[:5]
        before_refs = refs[len(operands) - len(before) : len(operands)]
        trace_ref, level_ref, gram_ref, projected_ref, external_ref = refs[-5:]

        def advance(j, _):
            at = pl.ds(pl.multiple_of(j * chunk, chunk), chunk)
            level = s_ref[:, at].astype(f32)
            if not first:
                level = cellular_leak_multiplier * refs[5][:, at] + level
            level_ref[:, at] = level
            trace_ref[:, at] = level.astype(bf16)
            return 0

        lax.fori_loop(0, senders // chunk, advance, 0)
        x = trace_ref[...]
        for t, ref in enumerate(list(before_refs) + [trace_ref]):
            gram_ref[:, t * batch : (t + 1) * batch] = lax.dot_general(
                x, ref[...], (((1,), (1,)), ((), ())), preferred_element_type=f32
            )
        projected_ref[...] = jnp.dot(own_ref[...], readout_ref[...], preferred_element_type=f32)
        external_ref[...] = jnp.dot(inputs_ref[t].astype(bf16), w_in_ref[...], preferred_element_type=f32)

    return pl.pallas_call(
        kernel,
        in_specs=[RESIDENT] * len(operands) + [UNREAD] * len(after),
        out_specs=[RESIDENT] * 5,
        out_shape=[
            pltpu.VMEM((batch, senders), bf16),
            pltpu.VMEM((batch, senders), f32),
            pltpu.VMEM((batch, steps * batch), f32),
            pltpu.VMEM((batch, outputs_n), f32),
            pltpu.VMEM(spikes.shape, f32),
        ],
        compiler_params=params(8),
        cost_estimate=cost(2 * batch * batch * senders * (steps + 3)),
        name="step_trace",
    )(*operands, *after)


def split_projections(where, projected, spikes, readout_own, rows):
    batch, outputs_n = projected[0].shape
    steps = len(projected) + 1
    share = steps // rows
    half = (rows // 2, share, batch, outputs_n)

    def kernel(where_ref, own_ref, readout_ref, *refs):
        keep_ref, send_ref, pool = refs[-3:]
        row = where_ref[0]
        for t in range(steps - 1):
            pool[t // share, t % share] = refs[t][...]
        pool[(steps - 1) // share, (steps - 1) % share] = jnp.dot(
            own_ref[...], readout_ref[...], preferred_element_type=f32
        )
        for j in range(rows // 2):
            keep_ref[j] = pool[row ^ (2 * j)]
            send_ref[j] = pool[row ^ (2 * j + 1)]

    return pl.pallas_call(
        kernel,
        in_specs=[SCALARS] + [RESIDENT] * (steps + 1),
        out_specs=[RESIDENT] * 2,
        out_shape=[pltpu.VMEM(half, f32)] * 2,
        scratch_shapes=[pltpu.VMEM((rows, share, batch, outputs_n), f32)],
        compiler_params=params(6),
        cost_estimate=cost(2 * batch * spikes.shape[1] * outputs_n),
        name="split_projections",
    )(where, spikes, readout_own, *projected)


def make_factors(where, projected, targets, feedback, fired, gain, decay, grams, groups, own):
    steps, batch, channels = targets.shape
    rows_all = steps * batch
    receivers = feedback.shape[1]
    width = groups * own
    tile = LANES // own
    lanes = tile * width
    share = projected[0].shape[0]
    count, held = len(projected), len(fired)

    def kernel(where_ref, *refs):
        proj_refs, refs = refs[:count], refs[count:]
        targets_ref, feedback_ref, refs = refs[0], refs[1], refs[2:]
        fired_refs, refs = refs[:held], refs[held:]
        gain_ref, decay_ref, refs = refs[0], refs[1], refs[2:]
        gram_refs, refs = refs[:steps], refs[steps:]
        readout_ref, factors_ref, squares_ref, pool, pair, own_gram, spread = refs
        g = pl.program_id(0)
        at = pl.ds(pl.multiple_of(g * lanes, lanes), lanes)
        row, col = where_ref[0], where_ref[1]

        @pl.when(g == 0)
        def _():
            for k in range(count):
                pool[row ^ k] = proj_refs[k][...]
            level = jnp.zeros((batch, channels), f32)
            for t in range(steps):
                level = readout_decay * level + pool[t // share, t % share]
                readout_ref[t] = level
                error = jax.nn.sigmoid(level) - targets_ref[t].astype(f32)
                high = error.astype(bf16)
                low = (error - high.astype(f32)).astype(bf16)
                pair[t * batch : (t + 1) * batch, :channels] = high
                pair[t * batch : (t + 1) * batch, channels:] = low

        some = pl.ds(pl.multiple_of(g * LANES, LANES), LANES)
        for t in range(steps):
            for k in range(groups):
                spread[t, col ^ k] = fired_refs[t * groups + k][:, some]
        half = feedback_ref[:, at]
        twice = jnp.concatenate([half, half], axis=0)
        gain_now, decay_now = gain_ref[:, at], decay_ref[:, at]
        future = jnp.zeros((batch, lanes), f32)
        for t in reversed(range(steps)):
            signal = jnp.dot(pair[t * batch : (t + 1) * batch, :], twice, preferred_element_type=f32)
            f = jnp.concatenate(
                [spread[t, c, :, i * own : (i + 1) * own] for i in range(tile) for c in range(groups)], axis=1
            ).astype(f32)
            slope = f * (1.0 - f)
            weighted = signal * slope
            strength = gain_now * slope
            factors_ref[t * batch : (t + 1) * batch, at] = (weighted - strength * future).astype(bf16)
            future = weighted + (decay_now - strength) * future
        for t in range(steps):
            to, upto = slice(t * batch, (t + 1) * batch), (t + 1) * batch
            gram = lax.dot_general(
                factors_ref[to, at], factors_ref[:upto, at], (((1,), (1,)), ((), ())), preferred_element_type=f32
            )

            @pl.when(g == 0)
            def _():
                own_gram[to, :upto] = gram

            @pl.when(g > 0)
            def _():
                own_gram[to, :upto] += gram

        @pl.when(g == pl.num_programs(0) - 1)
        def _():
            total = jnp.zeros((batch, batch), f32)
            for t in range(steps):
                for other in range(t + 1):
                    rows_t, cols = slice(t * batch, (t + 1) * batch), slice(other * batch, (other + 1) * batch)
                    value = own_gram[rows_t, cols] * gram_refs[t][:, cols]
                    total = total + (value if other == t else 2.0 * value)
            squares_ref[...] = jnp.full(squares_ref.shape, jnp.sum(total), f32)

    return pl.pallas_call(
        kernel,
        grid=(receivers // lanes,),
        in_specs=[SCALARS]
        + [RESIDENT] * count
        + [RESIDENT] * (4 + held)
        + [RESIDENT] * steps,
        out_specs=[whole_spec(targets.shape), RESIDENT, RESIDENT],
        out_shape=[
            jax.ShapeDtypeStruct(targets.shape, f32),
            pltpu.VMEM((rows_all, receivers), bf16),
            pltpu.VMEM((8, LANES), f32),
        ],
        scratch_shapes=[
            pltpu.VMEM((count,) + projected[0].shape, f32),
            pltpu.VMEM((rows_all, 2 * channels), bf16),
            pltpu.VMEM((rows_all, rows_all), f32),
            pltpu.VMEM((steps, groups, batch, LANES), bf16),
        ],
        compiler_params=params(24),
        cost_estimate=cost(2 * rows_all * rows_all * receivers),
        name="make_factors",
    )(where, *projected, targets, feedback, *fired, gain, decay, *grams)


def make_gradient(squares, limit, traces, factors, rows):
    batch, senders = traces[0].shape
    rows_all, receivers = factors.shape
    width = receivers // rows
    block = min(512, senders)
    count = len(traces)

    def kernel(squares_ref, factors_ref, *refs):
        o_ref, held = refs[count], refs[count + 1]
        at = pl.ds(pl.multiple_of(pl.program_id(0) * block, block), block)
        for t in range(count):
            held[t * batch : (t + 1) * batch, :] = refs[t][:, at]
        total = squares_ref[0:1, 0:1]
        clip = jnp.minimum(1.0, limit / jnp.sqrt(total + 1e-06))

        def columns(j, _):
            lanes = pl.ds(pl.multiple_of(j * 8 * width, 8 * width), 8 * width)
            product = lax.dot_general(
                held[...], factors_ref[:, lanes], (((0,), (0,)), ((), ())), preferred_element_type=f32
            )
            o_ref[:, pl.ds(pl.multiple_of(j * 8, 8), 8), :] = (product * clip).reshape(block, 8, width)
            return 0

        lax.fori_loop(0, rows // 8, columns, 0)

    return pl.pallas_call(
        kernel,
        grid=(senders // block,),
        in_specs=[RESIDENT] * (2 + count),
        out_specs=pl.BlockSpec((block, rows, width), lambda i: (i, 0, 0)),
        out_shape=jax.ShapeDtypeStruct((senders, rows, width), f32),
        scratch_shapes=[pltpu.VMEM((rows_all, block), bf16)],
        compiler_params=params(32),
        cost_estimate=cost(2 * senders * rows_all * receivers, 4 * senders * receivers),
        name="make_gradient",
    )(squares, factors, *traces)


def body(row_count, col_count, inputs, targets, initial_spikes, w_in, w_rec, w_out, feedback, adapt_gain, adapt_decay):
    steps, batch, channels = inputs.shape
    own = w_rec.shape[1]
    rows = w_rec.shape[2]
    width = w_rec.shape[3]
    part = rows * own
    row, col = lax.axis_index("row"), lax.axis_index("col")
    where = jnp.stack([row, col]).astype(jnp.int32)

    def swap(x, axis, k):
        size = row_count if axis == "row" else col_count
        return lax.ppermute(x, axis, [(d, d ^ k) for d in range(size)])

    def gather_row(x):
        even = {0: x}
        for k in range(2, row_count, 2):
            even[k] = swap(x, "row", k)
        pieces = []
        for k in range(0, row_count, 2):
            pieces += [even[k], swap(even[k], "row", 1)]
        return pieces

    def sum_over(x, axis, shifts):
        total = x
        for k in shifts:
            total = total + swap(x, axis, k)
        return total

    def mine(array, axis):
        return lax.dynamic_slice_in_dim(array, col * own, own, axis)

    outputs_n = feedback.shape[0]
    w_in_own = mine(w_in, 2).reshape(channels, part)
    readout_own = mine(w_out, 1).reshape(part, outputs_n)
    gain, decay = mine(adapt_gain, 1).reshape(1, part), mine(adapt_decay, 1).reshape(1, part)
    every_gain, every_decay = adapt_gain.reshape(1, -1), adapt_decay.reshape(1, -1)
    spikes = mine(initial_spikes, 2).astype(bf16).reshape(batch, part)
    early = [w_in_own, readout_own, gain, decay, every_gain, every_decay, where]
    weights, feedback_flat = flatten_weights(w_rec.reshape(-1, rows, width), feedback, early)

    voltage = fatigue = level = None
    traces, grams, fired, projected, fresh = [], [], [], [], []
    for t in range(steps):
        spikes_all, kept, *leaving = step_matmul(where, gather_row(spikes), weights, col_count, own)
        arrived = [swap(x, "col", k + 1) for k, x in enumerate(leaving)]
        trace, level, gram, projection, external = step_trace(
            t, spikes_all, level, list(traces), spikes, readout_own, inputs, w_in_own, fresh
        )
        traces.append(trace)
        grams.append(gram)
        if t > 0:
            projected.append(projection)
        spikes, voltage, fatigue = step_state(
            [external, kept] + arrived, spikes, voltage, fatigue, gain, decay
        )
        fresh = [swap(spikes, "col", k) for k in range(1, col_count)]
        fired += [spikes] + fresh

    keep, leave = split_projections(where, projected, spikes, readout_own, row_count)
    halves = keep + swap(leave, "row", 1)
    total = halves[0]
    for j in range(1, row_count // 2):
        total = total + swap(halves[j], "row", 2 * j)
    over_cols = sum_over(total, "col", range(1, col_count))
    readout, factors, squares = make_factors(
        where,
        gather_row(over_cols),
        targets,
        feedback_flat,
        fired,
        every_gain,
        every_decay,
        grams,
        col_count,
        own,
    )
    norm = sum_over(squares, "row", (1,))
    norm = sum_over(norm, "row", range(2, row_count, 2))
    norm = sum_over(norm, "col", range(1, col_count))
    limit = w_rec.shape[0] * width / 16.0
    return (readout, make_gradient(norm, limit, traces, factors, rows).reshape(w_rec.shape))


def plain(inputs, targets, initial_spikes, w_in, w_rec, w_out, feedback, adapt_gain, adapt_decay):
    steps_count, batch, channels = inputs.shape
    own_cols = w_rec.shape[1]
    rows_loc = w_rec.shape[2]
    entire_column_set = w_rec.shape[3]
    col_start = lax.axis_index("col") * own_cols
    rows_all = steps_count * batch

    def own_part(array, axis_dim):
        return lax.dynamic_slice_in_dim(array, col_start, own_cols, axis_dim)

    def select_cols(array, axis_dim):
        return own_part(array, axis_dim)

    def combine_currents(partial_value):
        return lax.psum_scatter(partial_value, "col", scatter_dimension=2, tiled=True)

    weights = w_rec.reshape(w_rec.shape[0] * own_cols, rows_loc * entire_column_set)
    w_in_loc = select_cols(w_in, 2)
    state_cols = w_in_loc.shape[2]
    external = jnp.dot(
        inputs.reshape(rows_all, channels).astype(jnp.bfloat16),
        w_in_loc.reshape(channels, -1),
        preferred_element_type=jnp.float32,
    ).reshape(steps_count, batch, rows_loc, state_cols)
    coupling_magnitude = select_cols(adapt_gain, 1)
    retention = select_cols(adapt_decay, 1)
    start_spikes = select_cols(initial_spikes, 2).astype(jnp.bfloat16)

    def advance(state, drive_now):
        pulse_output, cellular_charge, barrier_shift_amount, sender_trace = state
        arrivals = lax.all_gather(pulse_output, "row", axis=1, tiled=True).reshape(batch, -1)
        sender_trace = cellular_leak_multiplier * sender_trace + arrivals.astype(jnp.float32)
        partial_value = jnp.dot(arrivals, weights, preferred_element_type=jnp.float32).reshape(
            batch, rows_loc, entire_column_set
        )
        current = drive_now + combine_currents(partial_value)
        spike_float = pulse_output.astype(jnp.float32)
        cellular_charge = cellular_leak_multiplier * cellular_charge + current - spike_float
        barrier_shift_amount = retention * barrier_shift_amount + spike_float
        present_emission_frequency = jax.nn.sigmoid(
            cellular_charge - 1.0 - coupling_magnitude * barrier_shift_amount
        )
        surrogate_slope = present_emission_frequency * (1.0 - present_emission_frequency)
        pulse_output = present_emission_frequency.astype(jnp.bfloat16)
        return (
            (pulse_output, cellular_charge, barrier_shift_amount, sender_trace),
            (sender_trace.astype(jnp.bfloat16), surrogate_slope, pulse_output),
        )

    zeros = jnp.zeros((batch, rows_loc, state_cols), jnp.float32)
    trace_zero = jnp.zeros((batch, weights.shape[0]), jnp.float32)
    _, (traces, slopes, spikes) = lax.scan(
        advance, (start_spikes, zeros, zeros, trace_zero), external
    )
    readout_loc = own_part(w_out, 1).reshape(rows_loc * own_cols, -1)
    projected = lax.psum(
        jnp.dot(spikes.reshape(rows_all, -1), readout_loc, preferred_element_type=jnp.float32),
        ("row", "col"),
    )
    outputs_n = readout_loc.shape[1]
    projected = projected.reshape(steps_count, batch, outputs_n)

    def smooth(level, incoming):
        level = readout_decay * level + incoming
        return (level, level)

    _, readout = lax.scan(smooth, jnp.zeros((batch, outputs_n), jnp.float32), projected)
    errors = (jax.nn.sigmoid(readout) - targets.astype(jnp.float32)).reshape(rows_all, outputs_n)
    err_high = errors.astype(jnp.bfloat16)
    err_low = (errors - err_high.astype(jnp.float32)).astype(jnp.bfloat16)
    feedback_loc = select_cols(feedback, 2).reshape(outputs_n, -1)
    signal = jnp.dot(err_high, feedback_loc, preferred_element_type=jnp.float32) + jnp.dot(
        err_low, feedback_loc, preferred_element_type=jnp.float32
    )
    signal = signal.reshape(steps_count, batch, rows_loc, state_cols)
    weighted = signal * slopes
    decays = retention - slopes * coupling_magnitude

    def backward(carried, inputs_now):
        weighted_now, decay_now = inputs_now
        return (weighted_now + decay_now * carried, carried)

    _, future = lax.scan(backward, zeros, (weighted, decays), reverse=True)
    factors = (weighted - coupling_magnitude * slopes * future).astype(jnp.bfloat16)
    traces_flat = traces.reshape(rows_all, -1)
    pieces = lax.all_gather(
        factors.reshape(rows_all, rows_loc, state_cols), "col", axis=2, tiled=True
    )
    product = lax.dot_general(
        traces_flat,
        pieces.reshape(rows_all, -1),
        (((0,), (0,)), ((), ())),
        preferred_element_type=jnp.float32,
    )
    grad = product.reshape(-1, rows_loc, pieces.shape[2])
    squares = lax.psum(jnp.sum(grad * grad), ("row", "col"))
    clip_factor = jnp.minimum(1.0, NA * NB / 16.0 / jnp.sqrt(squares + 1e-06))
    return (readout, (grad * clip_factor).reshape(w_rec.shape))


def power_of_two(n):
    return n > 1 and n & (n - 1) == 0


def solution(mesh):
    row_count, col_count = mesh.shape["row"], mesh.shape["col"]

    def choose(inputs, targets, initial_spikes, w_in, w_rec, *rest):
        steps, batch, channels = inputs.shape
        own, rows, width = w_rec.shape[1:]
        fits = (
            power_of_two(row_count)
            and power_of_two(col_count)
            and LANES % own == 0
            and (rows * own) % LANES == 0
            and rows % 8 == 0
            and width % LANES == 0
            and batch % 16 == 0
            and channels % LANES == 0
            and steps % row_count == 0
        )
        run = functools.partial(body, row_count, col_count) if fits else plain
        return run(inputs, targets, initial_spikes, w_in, w_rec, *rest)

    return jax.shard_map(
        choose,
        mesh=mesh,
        in_specs=(
            P(),
            P(),
            P(None, "row", None),
            P(None, "row", None),
            P(None, "col", "row", None),
            P("row", None, None),
            P(None, "row", None),
            P("row", None),
            P("row", None),
        ),
        out_specs=(P(), P(None, "col", "row", None)),
        check_vma=False,
    )
```

```python
import functools
import jax
import jax.numpy as jnp
from jax import lax
from jax.experimental import pallas as pl
from jax.experimental.pallas import tpu as pltpu
from jax.sharding import PartitionSpec as P


NA = 128
NB = 128


cellular_leak_multiplier = 0.8
readout_decay = 0.8
f32 = jnp.float32
bf16 = jnp.bfloat16
LANES = 128


def params(mib):
    return pltpu.CompilerParams(vmem_limit_bytes=mib << 20)


def cost(flops, moved=0):
    return pl.CostEstimate(flops=int(flops), transcendentals=0, bytes_accessed=int(moved))


def whole_spec(shape):
    return pl.BlockSpec(shape, lambda *_: (0,) * len(shape))


SCALARS = pl.BlockSpec(memory_space=pltpu.SMEM)


RESIDENT = pl.BlockSpec(memory_space=pltpu.VMEM)
UNREAD = pl.BlockSpec(memory_space=pl.ANY)


def flatten_weights(w, feedback, own, before):
    senders, rows, width = w.shape
    block = min(256, senders)

    def kernel(w_ref, feedback_ref, *refs):
        o_ref, flat_ref = refs[-2:]
        start = pl.multiple_of(pl.program_id(0) * block, block)
        flat = w_ref[...].reshape(block, rows * width)
        o_ref[pl.ds(start, block), :] = jnp.concatenate(
            [
                flat[:, i * width + c * own : i * width + (c + 1) * own]
                for c in range(width // own)
                for i in range(rows)
            ],
            axis=1,
        )

        @pl.when(pl.program_id(0) == 0)
        def _():
            flat_ref[...] = feedback_ref[...].reshape(flat_ref.shape)

    return pl.pallas_call(
        kernel,
        grid=(senders // block,),
        in_specs=[pl.BlockSpec((block, rows, width), lambda i: (i, 0, 0)), whole_spec(feedback.shape)]
        + [UNREAD] * len(before),
        out_specs=[RESIDENT, whole_spec((feedback.shape[0], rows * width))],
        out_shape=[
            pltpu.VMEM((senders, rows * width), bf16),
            jax.ShapeDtypeStruct((feedback.shape[0], rows * width), bf16),
        ],
        compiler_params=params(24),
        cost_estimate=cost(w.size * 500, w.size * 4),
        name="flatten_weights",
    )(w, feedback, *before)


def step_matmul(where, pieces, weights, groups):
    batch, part = pieces[0].shape
    senders = weights.shape[0]
    count = len(pieces)

    def kernel(where_ref, *refs):
        piece_refs, w_ref = refs[:count], refs[count]
        spikes_ref, outs, pool = refs[count + 1], refs[count + 2 : -1], refs[-1]
        row, col = where_ref[0], where_ref[1]
        for k in range(count):
            start = pl.multiple_of((row ^ k) * part, part)
            spikes_ref[:, pl.ds(start, part)] = piece_refs[k][...]

        def group(c, _):
            at = pl.ds(pl.multiple_of(c * part, part), part)
            pool[col ^ c] = jnp.dot(spikes_ref[...], w_ref[:, at], preferred_element_type=f32)
            return 0

        lax.fori_loop(0, groups, group, 0)
        for k in range(groups):
            outs[k][...] = pool[k].astype(outs[k].dtype)

    return pl.pallas_call(
        kernel,
        in_specs=[SCALARS] + [RESIDENT] * (count + 1),
        out_specs=[RESIDENT] * (groups + 1),
        out_shape=[pltpu.VMEM((batch, senders), bf16)]
        + [pltpu.VMEM((batch, part), f32 if k == 0 else bf16) for k in range(groups)],
        scratch_shapes=[pltpu.VMEM((groups, batch, part), f32)],
        compiler_params=params(8),
        cost_estimate=cost(2 * batch * weights.size),
        name="step_matmul",
    )(where, *pieces, weights)


def spread_lanes(col, pieces, pool, o_ref, own):
    groups, _, part = pool.shape
    for k in range(groups):
        pool[col ^ k] = pieces[k][...]
    wide = LANES // own * groups * own

    def some(g, _):
        at = pl.ds(pl.multiple_of(g * LANES, LANES), LANES)
        held = [pool[c, :, at] for c in range(groups)]
        o_ref[:, pl.ds(pl.multiple_of(g * wide, wide), wide)] = jnp.concatenate(
            [x[:, i * own : (i + 1) * own] for i in range(LANES // own) for x in held], axis=1
        )
        return 0

    lax.fori_loop(0, part // LANES, some, 0)


def spread_fired(where, pieces, own):
    batch, part = pieces[0].shape
    groups = len(pieces)

    def kernel(where_ref, *refs):
        spread_lanes(where_ref[1], refs[:groups], refs[-1], refs[groups], own)

    return pl.pallas_call(
        kernel,
        in_specs=[SCALARS] + [RESIDENT] * groups,
        out_specs=RESIDENT,
        out_shape=pltpu.VMEM((batch, groups * part), bf16),
        scratch_shapes=[pltpu.VMEM((groups, batch, part), bf16)],
        compiler_params=params(6),
        cost_estimate=cost(1000 * batch * part),
        name="spread_fired",
    )(where, *pieces)


def step_state(partials, spikes, voltage, fatigue, gain, decay):
    batch, part = spikes.shape
    count = len(partials)
    first = voltage is None
    states = [] if first else [voltage, fatigue]

    def kernel(*refs):
        s_ref, gain_ref, decay_ref = refs[count : count + 3]
        s_out, v_out, u_out = refs[-3:]
        current = refs[0][...]
        for ref in refs[1:count]:
            current = current + ref[...].astype(f32)
        s = s_ref[...].astype(f32)
        v, u = current - s, s
        if not first:
            v = cellular_leak_multiplier * refs[count + 3][...] + v
            u = decay_ref[...] * refs[count + 4][...] + u
        s_out[...] = jax.nn.sigmoid(v - 1.0 - gain_ref[...] * u).astype(bf16)
        v_out[...] = v
        u_out[...] = u

    return pl.pallas_call(
        kernel,
        in_specs=[RESIDENT] * (count + 3 + len(states)),
        out_specs=[RESIDENT] * 3,
        out_shape=[pltpu.VMEM((batch, part), d) for d in (bf16, f32, f32)],
        compiler_params=params(6),
        cost_estimate=cost(2000 * spikes.size),
        name="step_state",
    )(*partials, spikes, gain, decay, *states)


def step_trace(where, spikes_all, trace, before, spikes, readout_own, inputs, w_in_own, fresh, own):
    batch, senders = spikes_all.shape
    steps = len(before) + 1
    outputs_n = readout_own.shape[1]
    first = trace is None
    operands = [spikes_all, spikes, readout_own, inputs, w_in_own] + ([] if first else [trace]) + before
    groups, part = len(fresh), spikes.shape[1]
    chunk = min(512, senders)

    def kernel(where_ref, *refs):
        if groups:
            fresh_refs, laid_ref, pool = refs[len(operands) : len(operands) + groups], refs[-2], refs[-1]
            refs = refs[: len(operands)] + refs[len(operands) + groups : -2]
            spread_lanes(where_ref[1], fresh_refs, pool, laid_ref, own)
        s_ref, own_ref, readout_ref, inputs_ref, w_in_ref = refs[:5]
        before_refs = refs[len(operands) - len(before) : len(operands)]
        trace_ref, level_ref, gram_ref, projected_ref, external_ref = refs[-5:]

        def advance(j, _):
            at = pl.ds(pl.multiple_of(j * chunk, chunk), chunk)
            level = s_ref[:, at].astype(f32)
            if not first:
                level = cellular_leak_multiplier * refs[5][:, at] + level
            level_ref[:, at] = level
            trace_ref[:, at] = level.astype(bf16)
            return 0

        lax.fori_loop(0, senders // chunk, advance, 0)
        x = trace_ref[...]
        for t, ref in enumerate(list(before_refs) + [trace_ref]):
            gram_ref[:, t * batch : (t + 1) * batch] = lax.dot_general(
                x, ref[...], (((1,), (1,)), ((), ())), preferred_element_type=f32
            )
        projected_ref[...] = jnp.dot(own_ref[...], readout_ref[...], preferred_element_type=f32)
        external_ref[...] = jnp.dot(inputs_ref[t].astype(bf16), w_in_ref[...], preferred_element_type=f32)

    return pl.pallas_call(
        kernel,
        in_specs=[SCALARS] + [RESIDENT] * (len(operands) + groups),
        out_specs=[RESIDENT] * (5 + bool(groups)),
        out_shape=[
            pltpu.VMEM((batch, senders), bf16),
            pltpu.VMEM((batch, senders), f32),
            pltpu.VMEM((batch, steps * batch), f32),
            pltpu.VMEM((batch, outputs_n), f32),
            pltpu.VMEM(spikes.shape, f32),
        ]
        + [pltpu.VMEM((batch, groups * part), bf16)] * bool(groups),
        scratch_shapes=[pltpu.VMEM((groups, batch, part), bf16)] * bool(groups),
        compiler_params=params(8),
        cost_estimate=cost(2 * batch * batch * senders * (steps + 3)),
        name="step_trace",
    )(where, *operands, *fresh)


def split_projections(where, projected, spikes, readout_own, rows):
    batch, outputs_n = projected[0].shape
    steps = len(projected) + 1
    share = steps // rows
    half = (rows // 2, share, batch, outputs_n)

    def kernel(where_ref, own_ref, readout_ref, *refs):
        keep_ref, send_ref, pool = refs[-3:]
        row = where_ref[0]
        for t in range(steps - 1):
            pool[t // share, t % share] = refs[t][...]
        pool[(steps - 1) // share, (steps - 1) % share] = jnp.dot(
            own_ref[...], readout_ref[...], preferred_element_type=f32
        )
        for j in range(rows // 2):
            keep_ref[j] = pool[row ^ (2 * j)]
            send_ref[j] = pool[row ^ (2 * j + 1)]

    return pl.pallas_call(
        kernel,
        in_specs=[SCALARS] + [RESIDENT] * (steps + 1),
        out_specs=[RESIDENT] * 2,
        out_shape=[pltpu.VMEM(half, f32)] * 2,
        scratch_shapes=[pltpu.VMEM((rows, share, batch, outputs_n), f32)],
        compiler_params=params(6),
        cost_estimate=cost(2 * batch * spikes.shape[1] * outputs_n),
        name="split_projections",
    )(where, spikes, readout_own, *projected)


def make_factors(where, projected, targets, feedback, fired, gain, decay, grams, lanes):
    steps, batch, channels = targets.shape
    rows_all = steps * batch
    receivers = feedback.shape[1]
    share = projected[0].shape[0]
    count, held = len(projected), len(fired)
    middle = steps // 2 * batch

    def kernel(where_ref, *refs):
        proj_refs, refs = refs[:count], refs[count:]
        targets_ref, feedback_ref, refs = refs[0], refs[1], refs[2:]
        fired_refs, refs = refs[:held], refs[held:]
        gain_ref, decay_ref, refs = refs[0], refs[1], refs[2:]
        gram_refs, refs = refs[:steps], refs[steps:]
        readout_ref, factors_ref, squares_ref, pool, pair, own_gram, signals = refs
        g = pl.program_id(0)
        at = pl.ds(pl.multiple_of(g * lanes, lanes), lanes)
        row = where_ref[0]

        @pl.when(g == 0)
        def _():
            for k in range(count):
                pool[row ^ k] = proj_refs[k][...]
            level = jnp.zeros((batch, channels), f32)
            for t in range(steps):
                level = readout_decay * level + pool[t // share, t % share]
                readout_ref[t] = level
                error = jax.nn.sigmoid(level) - targets_ref[t].astype(f32)
                high = error.astype(bf16)
                low = (error - high.astype(f32)).astype(bf16)
                pair[t * batch : (t + 1) * batch, :channels] = high
                pair[t * batch : (t + 1) * batch, channels:] = low

        half = feedback_ref[:, at]
        twice = jnp.concatenate([half, half], axis=0)
        gain_now, decay_now = gain_ref[:, at], decay_ref[:, at]
        signals[...] = jnp.dot(pair[...], twice, preferred_element_type=f32)
        future = jnp.zeros((batch, lanes), f32)
        for t in reversed(range(steps)):
            f = fired_refs[t][:, at].astype(f32)
            slope = f * (1.0 - f)
            weighted = signals[t * batch : (t + 1) * batch, :] * slope
            strength = gain_now * slope
            factors_ref[t * batch : (t + 1) * batch, at] = (weighted - strength * future).astype(bf16)
            future = weighted + (decay_now - strength) * future
        for to, upto in ((slice(0, middle), middle), (slice(middle, rows_all), rows_all)):
            gram = lax.dot_general(
                factors_ref[to, at], factors_ref[:upto, at], (((1,), (1,)), ((), ())), preferred_element_type=f32
            )

            @pl.when(g == 0)
            def _():
                own_gram[to, :upto] = gram

            @pl.when(g > 0)
            def _():
                own_gram[to, :upto] += gram

        @pl.when(g == pl.num_programs(0) - 1)
        def _():
            total = jnp.zeros((batch, batch), f32)
            for t in range(steps):
                for other in range(t + 1):
                    rows_t, cols = slice(t * batch, (t + 1) * batch), slice(other * batch, (other + 1) * batch)
                    value = own_gram[rows_t, cols] * gram_refs[t][:, cols]
                    total = total + (value if other == t else 2.0 * value)
            squares_ref[...] = jnp.full(squares_ref.shape, jnp.sum(total), f32)

    return pl.pallas_call(
        kernel,
        grid=(receivers // lanes,),
        in_specs=[SCALARS]
        + [RESIDENT] * count
        + [RESIDENT] * (4 + held)
        + [RESIDENT] * steps,
        out_specs=[whole_spec(targets.shape), RESIDENT, RESIDENT],
        out_shape=[
            jax.ShapeDtypeStruct(targets.shape, f32),
            pltpu.VMEM((rows_all, receivers), bf16),
            pltpu.VMEM((8, LANES), f32),
        ],
        scratch_shapes=[
            pltpu.VMEM((count,) + projected[0].shape, f32),
            pltpu.VMEM((rows_all, 2 * channels), bf16),
            pltpu.VMEM((rows_all, rows_all), f32),
            pltpu.VMEM((rows_all, lanes), f32),
        ],
        compiler_params=params(24),
        cost_estimate=cost(2 * rows_all * rows_all * receivers),
        name="make_factors",
    )(where, *projected, targets, feedback, *fired, gain, decay, *grams)


def make_gradient(squares, limit, traces, factors, rows):
    batch, senders = traces[0].shape
    rows_all, receivers = factors.shape
    width = receivers // rows
    block = min(512, senders)
    count = len(traces)

    def kernel(squares_ref, factors_ref, *refs):
        o_ref, held = refs[count], refs[count + 1]
        at = pl.ds(pl.multiple_of(pl.program_id(0) * block, block), block)
        for t in range(count):
            held[t * batch : (t + 1) * batch, :] = refs[t][:, at]
        total = squares_ref[0:1, 0:1]
        clip = jnp.minimum(1.0, limit / jnp.sqrt(total + 1e-06))

        def columns(j, _):
            lanes = pl.ds(pl.multiple_of(j * 8 * width, 8 * width), 8 * width)
            product = lax.dot_general(
                held[...], factors_ref[:, lanes], (((0,), (0,)), ((), ())), preferred_element_type=f32
            )
            o_ref[:, pl.ds(pl.multiple_of(j * 8, 8), 8), :] = (product * clip).reshape(block, 8, width)
            return 0

        lax.fori_loop(0, rows // 8, columns, 0)

    return pl.pallas_call(
        kernel,
        grid=(senders // block,),
        in_specs=[RESIDENT] * (2 + count),
        out_specs=pl.BlockSpec((block, rows, width), lambda i: (i, 0, 0)),
        out_shape=jax.ShapeDtypeStruct((senders, rows, width), f32),
        scratch_shapes=[pltpu.VMEM((rows_all, block), bf16)],
        compiler_params=params(32),
        cost_estimate=cost(2 * senders * rows_all * receivers, 4 * senders * receivers),
        name="make_gradient",
    )(squares, factors, *traces)


def body(row_count, col_count, inputs, targets, initial_spikes, w_in, w_rec, w_out, feedback, adapt_gain, adapt_decay):
    steps, batch, channels = inputs.shape
    own = w_rec.shape[1]
    rows = w_rec.shape[2]
    width = w_rec.shape[3]
    part = rows * own
    row, col = lax.axis_index("row"), lax.axis_index("col")
    where = jnp.stack([row, col]).astype(jnp.int32)

    def swap(x, axis, k):
        size = row_count if axis == "row" else col_count
        return lax.ppermute(x, axis, [(d, d ^ k) for d in range(size)])

    def gather_row(x):
        even = {0: x}
        for k in range(2, row_count, 2):
            even[k] = swap(x, "row", k)
        pieces = []
        for k in range(0, row_count, 2):
            pieces += [even[k], swap(even[k], "row", 1)]
        return pieces

    def sum_over(x, axis, shifts):
        total = x
        for k in shifts:
            total = total + swap(x, axis, k)
        return total

    def mine(array, axis):
        return lax.dynamic_slice_in_dim(array, col * own, own, axis)

    outputs_n = feedback.shape[0]
    w_in_own = mine(w_in, 2).reshape(channels, part)
    readout_own = mine(w_out, 1).reshape(part, outputs_n)
    gain, decay = mine(adapt_gain, 1).reshape(1, part), mine(adapt_decay, 1).reshape(1, part)
    every_gain, every_decay = adapt_gain.reshape(1, -1), adapt_decay.reshape(1, -1)
    spikes = mine(initial_spikes, 2).astype(bf16).reshape(batch, part)
    early = [w_in_own, readout_own, gain, decay, every_gain, every_decay, where]
    weights, feedback_flat = flatten_weights(w_rec.reshape(-1, rows, width), feedback, own, early)

    def spread_col(x):
        return [x] + [swap(x, "col", k) for k in range(1, col_count)]

    voltage = fatigue = level = None
    traces, grams, fired, projected, fresh = [], [], [], [], []
    for t in range(steps):
        pieces = gather_row(spikes)
        if t > 0:
            fresh = spread_col(spikes)
        spikes_all, kept, *leaving = step_matmul(where, pieces, weights, col_count)
        arrived = []
        for k, x in enumerate(leaving):
            arrived.append(swap(x, "col", k + 1))
        trace, level, gram, projection, external, *laid = step_trace(
            where, spikes_all, level, list(traces), spikes, readout_own, inputs, w_in_own, fresh, own
        )
        traces.append(trace)
        grams.append(gram)
        fired += laid
        if t > 0:
            projected.append(projection)
        spikes, voltage, fatigue = step_state(
            [external, kept] + arrived, spikes, voltage, fatigue, gain, decay
        )

    keep, leave = split_projections(where, projected, spikes, readout_own, row_count)
    halves = keep + swap(leave, "row", 1)
    total = halves[0]
    for j in range(1, row_count // 2):
        incoming = swap(halves[j], "row", 2 * j)
        total = total + incoming
    fired.append(spread_fired(where, spread_col(spikes), own))
    over_cols = sum_over(total, "col", range(1, col_count))
    readout, factors, squares = make_factors(
        where,
        gather_row(over_cols),
        targets,
        feedback_flat,
        fired,
        every_gain,
        every_decay,
        grams,
        LANES // own * width,
    )
    norm = sum_over(squares, "row", (1,))
    norm = sum_over(norm, "row", range(2, row_count, 2))
    norm = sum_over(norm, "col", range(1, col_count))
    limit = w_rec.shape[0] * width / 16.0
    return (readout, make_gradient(norm, limit, traces, factors, rows).reshape(w_rec.shape))


def plain(inputs, targets, initial_spikes, w_in, w_rec, w_out, feedback, adapt_gain, adapt_decay):
    steps_count, batch, channels = inputs.shape
    own_cols = w_rec.shape[1]
    rows_loc = w_rec.shape[2]
    entire_column_set = w_rec.shape[3]
    col_start = lax.axis_index("col") * own_cols
    rows_all = steps_count * batch

    def own_part(array, axis_dim):
        return lax.dynamic_slice_in_dim(array, col_start, own_cols, axis_dim)

    def select_cols(array, axis_dim):
        return own_part(array, axis_dim)

    def combine_currents(partial_value):
        return lax.psum_scatter(partial_value, "col", scatter_dimension=2, tiled=True)

    weights = w_rec.reshape(w_rec.shape[0] * own_cols, rows_loc * entire_column_set)
    w_in_loc = select_cols(w_in, 2)
    state_cols = w_in_loc.shape[2]
    external = jnp.dot(
        inputs.reshape(rows_all, channels).astype(jnp.bfloat16),
        w_in_loc.reshape(channels, -1),
        preferred_element_type=jnp.float32,
    ).reshape(steps_count, batch, rows_loc, state_cols)
    coupling_magnitude = select_cols(adapt_gain, 1)
    retention = select_cols(adapt_decay, 1)
    start_spikes = select_cols(initial_spikes, 2).astype(jnp.bfloat16)

    def advance(state, drive_now):
        pulse_output, cellular_charge, barrier_shift_amount, sender_trace = state
        arrivals = lax.all_gather(pulse_output, "row", axis=1, tiled=True).reshape(batch, -1)
        sender_trace = cellular_leak_multiplier * sender_trace + arrivals.astype(jnp.float32)
        partial_value = jnp.dot(arrivals, weights, preferred_element_type=jnp.float32).reshape(
            batch, rows_loc, entire_column_set
        )
        current = drive_now + combine_currents(partial_value)
        spike_float = pulse_output.astype(jnp.float32)
        cellular_charge = cellular_leak_multiplier * cellular_charge + current - spike_float
        barrier_shift_amount = retention * barrier_shift_amount + spike_float
        present_emission_frequency = jax.nn.sigmoid(
            cellular_charge - 1.0 - coupling_magnitude * barrier_shift_amount
        )
        surrogate_slope = present_emission_frequency * (1.0 - present_emission_frequency)
        pulse_output = present_emission_frequency.astype(jnp.bfloat16)
        return (
            (pulse_output, cellular_charge, barrier_shift_amount, sender_trace),
            (sender_trace.astype(jnp.bfloat16), surrogate_slope, pulse_output),
        )

    zeros = jnp.zeros((batch, rows_loc, state_cols), jnp.float32)
    trace_zero = jnp.zeros((batch, weights.shape[0]), jnp.float32)
    _, (traces, slopes, spikes) = lax.scan(
        advance, (start_spikes, zeros, zeros, trace_zero), external
    )
    readout_loc = own_part(w_out, 1).reshape(rows_loc * own_cols, -1)
    projected = lax.psum(
        jnp.dot(spikes.reshape(rows_all, -1), readout_loc, preferred_element_type=jnp.float32),
        ("row", "col"),
    )
    outputs_n = readout_loc.shape[1]
    projected = projected.reshape(steps_count, batch, outputs_n)

    def smooth(level, incoming):
        level = readout_decay * level + incoming
        return (level, level)

    _, readout = lax.scan(smooth, jnp.zeros((batch, outputs_n), jnp.float32), projected)
    errors = (jax.nn.sigmoid(readout) - targets.astype(jnp.float32)).reshape(rows_all, outputs_n)
    err_high = errors.astype(jnp.bfloat16)
    err_low = (errors - err_high.astype(jnp.float32)).astype(jnp.bfloat16)
    feedback_loc = select_cols(feedback, 2).reshape(outputs_n, -1)
    signal = jnp.dot(err_high, feedback_loc, preferred_element_type=jnp.float32) + jnp.dot(
        err_low, feedback_loc, preferred_element_type=jnp.float32
    )
    signal = signal.reshape(steps_count, batch, rows_loc, state_cols)
    weighted = signal * slopes
    decays = retention - slopes * coupling_magnitude

    def backward(carried, inputs_now):
        weighted_now, decay_now = inputs_now
        return (weighted_now + decay_now * carried, carried)

    _, future = lax.scan(backward, zeros, (weighted, decays), reverse=True)
    factors = (weighted - coupling_magnitude * slopes * future).astype(jnp.bfloat16)
    traces_flat = traces.reshape(rows_all, -1)
    pieces = lax.all_gather(
        factors.reshape(rows_all, rows_loc, state_cols), "col", axis=2, tiled=True
    )
    product = lax.dot_general(
        traces_flat,
        pieces.reshape(rows_all, -1),
        (((0,), (0,)), ((), ())),
        preferred_element_type=jnp.float32,
    )
    grad = product.reshape(-1, rows_loc, pieces.shape[2])
    squares = lax.psum(jnp.sum(grad * grad), ("row", "col"))
    clip_factor = jnp.minimum(1.0, NA * NB / 16.0 / jnp.sqrt(squares + 1e-06))
    return (readout, (grad * clip_factor).reshape(w_rec.shape))


def power_of_two(n):
    return n > 1 and n & (n - 1) == 0


def solution(mesh):
    row_count, col_count = mesh.shape["row"], mesh.shape["col"]

    def choose(inputs, targets, initial_spikes, w_in, w_rec, *rest):
        steps, batch, channels = inputs.shape
        own, rows, width = w_rec.shape[1:]
        fits = (
            power_of_two(row_count)
            and power_of_two(col_count)
            and LANES % own == 0
            and (rows * own) % LANES == 0
            and rows % 8 == 0
            and width % LANES == 0
            and batch % 16 == 0
            and channels % LANES == 0
            and steps % row_count == 0
        )
        run = functools.partial(body, row_count, col_count) if fits else plain
        return run(inputs, targets, initial_spikes, w_in, w_rec, *rest)

    return jax.shard_map(
        choose,
        mesh=mesh,
        in_specs=(
            P(),
            P(),
            P(None, "row", None),
            P(None, "row", None),
            P(None, "col", "row", None),
            P("row", None, None),
            P(None, "row", None),
            P("row", None),
            P("row", None),
        ),
        out_specs=(P(), P(None, "col", "row", None)),
        check_vma=False,
    )
```
